32 devices in a mesh: head: 4 (over z), outer: 2 (over core), inner: 4 (over y, x).
Axes of the slice: x: 2, y: 2, z: 4, core: 2. Of those that a mesh axis runs over, the one named last changes fastest.
Arguments:
- query: bfloat16 [2048, 64, 128], P(('outer', 'inner'), 'head'), may hold values from -24 to 24
- keys: bfloat16 [2048, 8, 128], P(('outer', 'inner'), 'head'), may hold values from -8 to 8
- values: bfloat16 [2048, 8, 128], P(('outer', 'inner'), 'head'), may hold values from -6 to 6
- forward_output: bfloat16 [2048, 64, 128], P(('outer', 'inner'), 'head'), may hold values from -2.390625 to 2.390625
- d_out: bfloat16 [2048, 64, 128], P(('outer', 'inner'), 'head'), may hold values from -2.390625 to 2.390625
- span_order: int32 [1, 8], replicated, may hold values from 0 to 7, each once within a row
Outputs:
- d_query: bfloat16 [8, 256, 64, 128], P(('outer', 'inner'), 'head')
- key_gradient: bfloat16 [8, 256, 8, 128], P(('outer', 'inner'), 'head')
- value_gradient: bfloat16 [8, 256, 8, 128], P(('outer', 'inner'), 'head')
The draws below stay inside these ranges and needn't reach their ends.
Inputs may be any that keep to these rules, and one draw needn't show every extreme that they name: `span_order`: each row holds every number once.
All inputs are finite; a program needn't handle non-finite values.
Results may differ from the reference program's by a relative error of at most 0.0051.
Values may be sent and summed in bfloat16 or wider, within the bound.
No kernel may reach another device: no remote copies, remote signals or barrier semaphores. Data moves between devices by JAX's collectives and lax.ppermute only.
A program may use at most 64 MiB of HBM per device.

```python
import jax
import jax.numpy as jnp
from jax import lax

QUERY_HEADS = 64
KEY_VALUE_HEADS = 8
HEAD_SIZE = 128
BLOCK_ROWS = 256
SEQUENCE_BLOCKS = 8
SEQUENCE_COUNT = 1
SEQUENCE_TOKENS = 2048


def draw_keys(key, part):
    row_total = SEQUENCE_COUNT * SEQUENCE_TOKENS
    sampled_rows = jnp.clip(jax.random.normal(jax.random.fold_in(key, 19), (row_total, KEY_VALUE_HEADS, HEAD_SIZE), jnp.float32), -8.0, 8.0)
    return sampled_rows.astype(jnp.bfloat16)


def draw_query(key, part):
    row_total = SEQUENCE_COUNT * SEQUENCE_TOKENS
    sampled_rows = jnp.clip(jax.random.normal(jax.random.fold_in(key, 29), (row_total, QUERY_HEADS, HEAD_SIZE), jnp.float32), -8.0, 8.0)
    return sampled_rows.astype(jnp.bfloat16)


def block_levels(stream_key, extent, cuts, smallest, largest):
    level, own = 1.0, jax.random.fold_in(stream_key, 6)
    for dim, parts in cuts:
        draws = jnp.exp(jax.random.uniform(jax.random.fold_in(own, dim), (parts,), jnp.float32, smallest / len(cuts), largest / len(cuts)))
        level = level * jnp.repeat(draws, extent[dim] // parts).reshape([-1 if axis == dim else 1 for axis in range(len(extent))])
    return level


def normal_values(rng, shape, deviation, limit, pieces=(), kind=jnp.bfloat16):
    result = jax.random.normal(rng, shape, jnp.float32) * deviation
    if len(pieces) > 0:
        result = block_levels(rng, shape, pieces, -0.22, 0.18) * result
    return jnp.clip(result, min=-limit, max=limit).astype(kind)


def setup_inputs(seed: int = 0) -> dict:
    streams_of = jax.random.split(jax.random.key(seed), 7)
    return {
        "query": draw_query(jax.random.fold_in(streams_of[6], 71), 0),
        "keys": draw_keys(jax.random.fold_in(streams_of[6], 71), 0),
        "values": normal_values(streams_of[2], (SEQUENCE_COUNT * SEQUENCE_TOKENS, KEY_VALUE_HEADS, HEAD_SIZE), 1.0, 6.0, ((0, 8), (1, 4))),
        "forward_output": normal_values(streams_of[3], (SEQUENCE_COUNT * SEQUENCE_TOKENS, QUERY_HEADS, HEAD_SIZE), 0.3, 2.390625, ((0, 8), (1, 4))),
        "d_out": normal_values(streams_of[4], (SEQUENCE_COUNT * SEQUENCE_TOKENS, QUERY_HEADS, HEAD_SIZE), 0.3, 2.390625, ((0, 8), (1, 4))),
        "span_order": jax.vmap(lambda own: jax.random.permutation(own, SEQUENCE_BLOCKS))(jax.random.split(streams_of[5], SEQUENCE_COUNT)).reshape((SEQUENCE_COUNT, SEQUENCE_BLOCKS)).astype(jnp.int32),
    }


def one_sequence(block_pieces):
    query, keys, values, forward_output, d_out, order_row = block_pieces
    score_scale = HEAD_SIZE ** -0.5
    group_members = QUERY_HEADS // KEY_VALUE_HEADS
    offsets = jnp.arange(BLOCK_ROWS, dtype=jnp.int32)
    position = (order_row[:, None] * BLOCK_ROWS + offsets[None, :]).reshape(SEQUENCE_TOKENS)
    visible = position[None, :] <= position[:, None]
    delta_all = jnp.sum(d_out.astype(jnp.float32) * forward_output.astype(jnp.float32), axis=-1)

    def one_head(head_id):
        group_id = head_id // group_members
        query_head = lax.dynamic_index_in_dim(query, head_id, 1, keepdims=False)
        key_head = lax.dynamic_index_in_dim(keys, group_id, 1, keepdims=False)
        value_head = lax.dynamic_index_in_dim(values, group_id, 1, keepdims=False)
        grad_head = lax.dynamic_index_in_dim(d_out, head_id, 1, keepdims=False)
        delta_head = lax.dynamic_index_in_dim(delta_all, head_id, 1, keepdims=False)
        scores = jnp.dot(query_head, key_head.T, preferred_element_type=jnp.float32) * score_scale
        scores = jnp.where(visible, scores, -jnp.inf)
        highest = jnp.max(scores, axis=1, keepdims=True)
        log_total = highest + jnp.log(jnp.sum(jnp.exp(scores - highest), axis=1, keepdims=True))
        weights = jnp.exp(scores - log_total)
        weights_low = weights.astype(jnp.bfloat16)
        d_weights = jnp.dot(grad_head, value_head.T, preferred_element_type=jnp.float32)
        d_scores = (weights * (d_weights - delta_head[:, None])).astype(jnp.bfloat16)
        grad_query = jnp.dot(d_scores, key_head, preferred_element_type=jnp.float32) * score_scale
        key_gradient_fn = jnp.dot(d_scores.T, query_head, preferred_element_type=jnp.float32) * score_scale
        value_gradient_fn = jnp.dot(weights_low.T, grad_head, preferred_element_type=jnp.float32)
        return grad_query, key_gradient_fn, value_gradient_fn

    grad_query, key_gradient_fn, value_gradient_fn = lax.map(one_head, jnp.arange(QUERY_HEADS, dtype=jnp.int32))
    grad_query = jnp.transpose(grad_query, (1, 0, 2))
    key_gradient_fn = jnp.transpose(jnp.sum(key_gradient_fn.reshape(KEY_VALUE_HEADS, group_members, SEQUENCE_TOKENS, HEAD_SIZE), axis=1), (1, 0, 2))
    value_gradient_fn = jnp.transpose(jnp.sum(value_gradient_fn.reshape(KEY_VALUE_HEADS, group_members, SEQUENCE_TOKENS, HEAD_SIZE), axis=1), (1, 0, 2))
    return (grad_query.astype(jnp.bfloat16), key_gradient_fn.astype(jnp.bfloat16), value_gradient_fn.astype(jnp.bfloat16))


def reference(query, keys, values, forward_output, d_out, span_order):
    block_pieces = (query.reshape(SEQUENCE_COUNT, SEQUENCE_TOKENS, QUERY_HEADS, HEAD_SIZE), keys.reshape(SEQUENCE_COUNT, SEQUENCE_TOKENS, KEY_VALUE_HEADS, HEAD_SIZE),
              values.reshape(SEQUENCE_COUNT, SEQUENCE_TOKENS, KEY_VALUE_HEADS, HEAD_SIZE), forward_output.reshape(SEQUENCE_COUNT, SEQUENCE_TOKENS, QUERY_HEADS, HEAD_SIZE),
              d_out.reshape(SEQUENCE_COUNT, SEQUENCE_TOKENS, QUERY_HEADS, HEAD_SIZE), span_order)
    grad_query, key_gradient_fn, value_gradient_fn = lax.map(one_sequence, block_pieces)
    d_query = grad_query.reshape(SEQUENCE_COUNT * SEQUENCE_BLOCKS, BLOCK_ROWS, QUERY_HEADS, HEAD_SIZE)
    key_gradient = key_gradient_fn.reshape(SEQUENCE_COUNT * SEQUENCE_BLOCKS, BLOCK_ROWS, KEY_VALUE_HEADS, HEAD_SIZE)
    value_gradient = value_gradient_fn.reshape(SEQUENCE_COUNT * SEQUENCE_BLOCKS, BLOCK_ROWS, KEY_VALUE_HEADS, HEAD_SIZE)
    return (d_query, key_gradient, value_gradient)
```

```python
import functools
import math

import jax
import jax.numpy as jnp
from jax import lax
from jax.experimental import pallas as pl
from jax.experimental.pallas import tpu as pltpu
from jax.sharding import PartitionSpec as P

F32 = jnp.float32
BF16 = jnp.bfloat16
NT = (((1,), (1,)), ((), ()))
NN = (((1,), (0,)), ((), ()))
MASKED = -1e30
VMEM = pl.BlockSpec(memory_space=pltpu.VMEM)
SMEM = pl.BlockSpec(memory_space=pltpu.SMEM)


def dot(a, b, dims):
    return lax.dot_general(a, b, dims, preferred_element_type=F32)


def causal_tile(rows):
    shape = (rows, rows)
    return lax.broadcasted_iota(jnp.int32, shape, 0) <= lax.broadcasted_iota(jnp.int32, shape, 1)


def over_visible(place, tile):
    tile(place, True)

    def turn(k, _):
        tile(k, False)
        return 0

    lax.fori_loop(0, place, turn, 0)


def lse_kernel(group, scale, table, q_ref, k_ref, lse_ref, m_ref, l_ref):
    slots, heads, rows, width = q_ref.shape
    scale2 = scale * math.log2(math.e)
    causal = causal_tile(rows)
    for s in range(slots):
        for g in range(0, heads, group):

            def tile(k, diag):
                keys = k_ref[table[1, k]]
                for j in range(g, g + group):
                    st = dot(keys, q_ref[s, j], NT)
                    if diag:
                        st = jnp.where(causal, st, MASKED)
                    st = st.reshape(rows // 8, 8, rows)
                    m_new = jnp.max(st, axis=0)
                    if not diag:
                        m_old = m_ref[j - g]
                        m_new = jnp.maximum(m_old, m_new)
                    total = jnp.sum(jnp.exp2((st - m_new[None]) * scale2), axis=0)
                    if not diag:
                        total = total + l_ref[j - g] * jnp.exp2((m_old - m_new) * scale2)
                    m_ref[j - g] = m_new
                    l_ref[j - g] = total

            over_visible(table[0, s], tile)
            for j in range(g, g + group):
                m = m_ref[j - g]
                high = jnp.max(m, axis=0, keepdims=True)
                total = jnp.sum(
                    l_ref[j - g] * jnp.exp2((m - high) * scale2), axis=0, keepdims=True
                )
                lse_ref[s, j : j + 1, :] = high * scale2 + jnp.log2(total)


def lse_call(table, q, k, group, scale):
    slots, heads, rows, width = q.shape
    flops = slots * heads * rows * rows * k.shape[0] * width
    return pl.pallas_call(
        functools.partial(lse_kernel, group, scale),
        out_shape=jax.ShapeDtypeStruct((slots, heads, rows), F32),
        in_specs=[SMEM, VMEM, VMEM],
        out_specs=VMEM,
        scratch_shapes=[pltpu.VMEM((group, 8, rows), F32)] * 2,
        cost_estimate=pl.CostEstimate(flops=flops, bytes_accessed=q.size * 2, transcendentals=0),
        name="lse",
    )(table, q, k)


def grad_kernel(
    group,
    scale,
    table,
    q_ref,
    do_ref,
    k_ref,
    kt_ref,
    v_ref,
    lse_ref,
    delta_ref,
    dq_ref,
    dk_ref,
    dv_ref,
    dqt_ref,
    dka_ref,
    dva_ref,
):
    slots, heads, rows, width = q_ref.shape
    scale2 = scale * math.log2(math.e)
    causal = causal_tile(rows)
    dka_ref[...] = jnp.zeros_like(dka_ref)
    dva_ref[...] = jnp.zeros_like(dva_ref)
    for s in range(slots):
        for g in range(0, heads, group):

            def tile(k, diag):
                block = table[1, k]
                keys = k_ref[block]
                keys_t = kt_ref[block]
                vals = v_ref[block]
                dk = dka_ref[block]
                dv = dva_ref[block]
                for j in range(g, g + group):
                    st = dot(keys, q_ref[s, j], NT)
                    dp = dot(vals, do_ref[s, j], NT)
                    p = jnp.exp2(st * scale2 - lse_ref[s, j : j + 1, :])
                    if diag:
                        p = jnp.where(causal, p, 0.0)
                    ds = (p * (dp - delta_ref[s, j : j + 1, :])).astype(BF16)
                    dv = dv + dot(p.astype(BF16), do_ref[s, j], NN)
                    dk = dk + dot(ds, q_ref[s, j], NN)
                    part = dot(keys_t, ds, NN)
                    if diag:
                        dqt_ref[j - g] = part
                    else:
                        dqt_ref[j - g] += part
                dka_ref[block] = dk
                dva_ref[block] = dv

            over_visible(table[0, s], tile)
            for j in range(g, g + group):
                dq_ref[s, j] = (dqt_ref[j - g] * scale).T.astype(BF16)
    dk_ref[...] = (dka_ref[...] * scale).astype(BF16)
    dv_ref[...] = dva_ref[...].astype(BF16)


def grad_call(table, q, do, k, kt, v, lse, delta, group, scale):
    slots, heads, rows, width = q.shape
    flops = 5 * slots * heads * rows * rows * k.shape[0] * width
    return pl.pallas_call(
        functools.partial(grad_kernel, group, scale),
        out_shape=[
            jax.ShapeDtypeStruct(q.shape, BF16),
            jax.ShapeDtypeStruct(k.shape, BF16),
            jax.ShapeDtypeStruct(k.shape, BF16),
        ],
        in_specs=[SMEM] + [VMEM] * 7,
        out_specs=[VMEM] * 3,
        scratch_shapes=[
            pltpu.VMEM((group, width, rows), F32),
            pltpu.VMEM(k.shape, F32),
            pltpu.VMEM(k.shape, F32),
        ],
        cost_estimate=pl.CostEstimate(flops=flops, bytes_accessed=q.size * 6, transcendentals=0),
        name="grads",
    )(table, q, do, k, kt, v, lse, delta)


def exchange(x, axes):
    return lax.all_to_all(x, axes, split_axis=0, concat_axis=0, tiled=True)


def body(query, keys, values, forward_output, d_out, span_order):
    rows, heads, width = query.shape
    kv_count = keys.shape[1]
    members = heads // kv_count
    scale = width ** (-0.5)
    cores, inner, zs = lax.axis_size("outer"), lax.axis_size("inner"), lax.axis_size("head")
    core, place = lax.axis_index("outer"), lax.axis_index("inner")
    blocks = cores * inner
    own_heads = heads // cores
    shared = kv_count % cores != 0
    own_kv = 1 if shared else kv_count // cores
    group_heads = own_heads // own_kv
    slice_rows = rows // zs

    def spread(x):
        x = jnp.transpose(x, (1, 0, 2))
        x = jnp.broadcast_to(x, (cores,) + x.shape) if shared else x.reshape(cores, own_kv, rows, width)
        x = jnp.broadcast_to(x[:, None], (cores, inner) + x.shape[1:])
        return x.reshape((blocks,) + x.shape[2:])

    k_all = exchange(spread(keys), ("outer", "inner"))
    v_all = exchange(spread(values), ("outer", "inner"))
    k_all, v_all = jnp.swapaxes(k_all, 0, 1), jnp.swapaxes(v_all, 0, 1)

    def share(x):
        x = jnp.moveaxis(x, 1, 0)
        return exchange(x.reshape((cores, own_heads) + x.shape[1:]), "outer")

    delta = jnp.sum(d_out.astype(F32) * forward_output.astype(F32), axis=-1)
    q_all, do_all, delta_all = share(query), share(d_out), share(delta)

    order = span_order[0]
    by_place = jnp.zeros((blocks,), jnp.int32).at[order].set(jnp.arange(blocks, dtype=jnp.int32))
    q_places = order[jnp.arange(cores) * inner + place]
    table = jnp.stack([jnp.pad(q_places, (0, blocks - cores)), by_place])

    dq, dk, dv = [], [], []
    group = min(8, group_heads)
    for g in range(own_kv):
        mine = slice(g * group_heads, (g + 1) * group_heads)
        q, do, delta_g = q_all[:, mine], do_all[:, mine], delta_all[:, mine]
        lse = lse_call(table, q, k_all[g], group, scale)
        parts = grad_call(
            table, q, do, k_all[g], jnp.swapaxes(k_all[g], 1, 2), v_all[g], lse, delta_g, group, scale
        )
        for kept, part in zip((dq, dk, dv), parts):
            kept.append(part)

    dq = jnp.concatenate(dq, axis=1).reshape(cores, own_heads, zs, slice_rows, width)
    dq = jnp.transpose(dq, (0, 2, 1, 3, 4)).reshape(cores * zs, own_heads, slice_rows, width)
    dq = exchange(dq, ("outer", "head")).reshape(cores, zs, own_heads, slice_rows, width)
    dq = jnp.transpose(dq, (3, 1, 0, 2, 4)).reshape(1, slice_rows, zs * heads, width)

    kv = jnp.stack([jnp.stack(dk), jnp.stack(dv)])
    kv = kv.reshape(2, own_kv, cores, inner, rows, width)
    kv = exchange(jnp.transpose(kv, (3, 0, 1, 2, 4, 5)), "inner")
    kv = jnp.sum(kv.astype(F32), axis=0)
    kv = kv.astype(BF16).reshape(2, own_kv, cores, zs, slice_rows, width)
    kv = jnp.transpose(kv, (2, 3, 0, 1, 4, 5)).reshape(cores * zs, 2, own_kv, slice_rows, width)
    kv = exchange(kv, ("outer", "head")).reshape(cores, zs, 2, own_kv, slice_rows, width)
    if shared:
        kv = jnp.sum(kv.astype(F32), axis=0, keepdims=True).astype(BF16)
    kv = jnp.transpose(kv, (2, 4, 1, 0, 3, 5)).reshape(2, 1, slice_rows, zs * kv_count, width)
    return dq, kv[0], kv[1]


def solution(mesh):
    rows_spec = P(("outer", "inner"), "head", None)
    out_spec = P(("outer", "inner"), "head", None, None)
    return jax.shard_map(
        body,
        mesh=mesh,
        in_specs=(rows_spec,) * 5 + (P(),),
        out_specs=(out_spec,) * 3,
        check_vma=False,
    )
```

```python
import functools
import math

import jax
import jax.numpy as jnp
from jax import lax
from jax.experimental import pallas as pl
from jax.experimental.pallas import tpu as pltpu
from jax.sharding import PartitionSpec as P


F32 = jnp.float32
BF16 = jnp.bfloat16
NT = (((1,), (1,)), ((), ()))
NN = (((1,), (0,)), ((), ()))
MASKED = -1e30
VMEM = pl.BlockSpec(memory_space=pltpu.VMEM)
SMEM = pl.BlockSpec(memory_space=pltpu.SMEM)


def dot(a, b, dims):
    return lax.dot_general(a, b, dims, preferred_element_type=F32)


def causal_tile(rows):
    shape = (rows, rows)
    return lax.broadcasted_iota(jnp.int32, shape, 0) <= lax.broadcasted_iota(jnp.int32, shape, 1)


def over_visible(place, tile):
    tile(place, True)

    def turn(k, _):
        tile(k, False)
        return 0

    lax.fori_loop(0, place, turn, 0)


def lse_kernel(group, scale, blocks, table, *refs):
    slots = (len(refs) - 3) // 2
    q_refs, kv_ref, lse_refs = refs[:slots], refs[slots], refs[slots + 1 : 2 * slots + 1]
    m_ref, l_ref = refs[-2:]
    heads, rows, _ = q_refs[0].shape
    scale2 = scale * math.log2(math.e)
    causal = causal_tile(rows)
    for q_ref, lse_ref, s in zip(q_refs, lse_refs, range(slots)):
        for g in range(0, heads, group):

            def tile(k, diag):
                keys = kv_ref[table[k], 0]
                for j in range(g, g + group):
                    st = dot(keys, q_ref[j], NT)
                    if diag:
                        st = jnp.where(causal, st, MASKED)
                    st = st.reshape(rows // 8, 8, rows)
                    m_new = jnp.max(st, axis=0)
                    if not diag:
                        m_old = m_ref[j - g]
                        m_new = jnp.maximum(m_old, m_new)
                    total = jnp.sum(jnp.exp2((st - m_new[None]) * scale2), axis=0)
                    if not diag:
                        total = total + l_ref[j - g] * jnp.exp2((m_old - m_new) * scale2)
                    m_ref[j - g] = m_new
                    l_ref[j - g] = total

            over_visible(table[blocks + s], tile)
            for j in range(g, g + group):
                m = m_ref[j - g]
                high = jnp.max(m, axis=0, keepdims=True)
                total = jnp.sum(
                    l_ref[j - g] * jnp.exp2((m - high) * scale2), axis=0, keepdims=True
                )
                lse_ref[j : j + 1, :] = high * scale2 + jnp.log2(total)


def lse_call(table, q, kv, group, scale):
    heads, rows, width = q[0].shape
    blocks = kv.shape[0]
    flops = len(q) * heads * rows * rows * blocks * width
    return pl.pallas_call(
        functools.partial(lse_kernel, group, scale, blocks),
        out_shape=[jax.ShapeDtypeStruct((heads, rows), F32)] * len(q),
        in_specs=[SMEM] + [VMEM] * (len(q) + 1),
        out_specs=[VMEM] * len(q),
        scratch_shapes=[pltpu.VMEM((group, 8, rows), F32)] * 2,
        cost_estimate=pl.CostEstimate(flops=flops, bytes_accessed=q[0].size * 4, transcendentals=0),
        name="lse",
    )(table, *q, kv)


def grad_kernel(group, scale, inner, slots, table, *refs):
    q_refs, do_refs, lse_refs, delta_refs = (refs[k * slots : (k + 1) * slots] for k in range(4))
    kv_ref, dq_ref = refs[4 * slots], refs[4 * slots + 1]
    out_refs = refs[4 * slots + 2 : 4 * slots + 2 + inner]
    kt_ref, dqt_ref, dka_ref, dva_ref = refs[-4:]
    heads, rows, _ = q_refs[0].shape
    blocks = kv_ref.shape[0]
    slice_rows = dq_ref.shape[2]
    zs = rows // slice_rows
    scale2 = scale * math.log2(math.e)
    causal = causal_tile(rows)
    core, place_in, z_in = (table[blocks + slots + k] for k in range(3))
    dka_ref[...] = jnp.zeros_like(dka_ref)
    dva_ref[...] = jnp.zeros_like(dva_ref)
    for b in range(blocks):
        kt_ref[b] = kv_ref[b, 0].T
    for s in range(slots):
        q_ref, do_ref, lse_ref, delta_ref = q_refs[s], do_refs[s], lse_refs[s], delta_refs[s]
        for g in range(0, heads, group):

            def tile(k, diag):
                block = table[k]
                keys, vals, keys_t = kv_ref[block, 0], kv_ref[block, 1], kt_ref[block]
                dk, dv = dka_ref[block], dva_ref[block]
                for j in range(g, g + group):
                    st = dot(keys, q_ref[j], NT)
                    dp = dot(vals, do_ref[j], NT)
                    p = jnp.exp2(st * scale2 - lse_ref[j : j + 1, :])
                    if diag:
                        p = jnp.where(causal, p, 0.0)
                    ds = (p * (dp - delta_ref[j : j + 1, :])).astype(BF16)
                    dv = dv + dot(p.astype(BF16), do_ref[j], NN)
                    dk = dk + dot(ds, q_ref[j], NN)
                    part = dot(keys_t, ds, NN)
                    if diag:
                        dqt_ref[j - g] = part
                    else:
                        dqt_ref[j - g] += part
                dka_ref[block] = dk
                dva_ref[block] = dv

            over_visible(table[blocks + s], tile)
            to_core = lax.rem(core + s, slots)
            for j in range(g, g + group):
                dq = (dqt_ref[j - g] * scale).T.astype(BF16)
                for z in range(zs):
                    dq_ref[to_core * zs + z, j] = dq[z * slice_rows : (z + 1) * slice_rows]
    for step, out_ref in enumerate(out_refs):
        for c in range(slots):
            block = partner(core, c, slots) * inner + partner(place_in, step, inner)
            for z in range(zs):
                start = pl.multiple_of(partner(z_in, z, zs) * slice_rows, slice_rows)
                cut = pl.ds(start, slice_rows)
                out_ref[c * zs + z, 0] = (dka_ref[block, cut] * scale).astype(BF16)
                out_ref[c * zs + z, 1] = dva_ref[block, cut].astype(BF16)


def grad_call(table, q, do, lse, delta, kv, group, scale, inner, zs):
    heads, rows, width = q[0].shape
    slots, blocks = len(q), kv.shape[0]
    slice_rows = rows // zs
    flops = 5 * slots * heads * rows * rows * blocks * width
    outs = [(slots * zs, heads, slice_rows, width)] + [(slots * zs, 2, slice_rows, width)] * inner
    return pl.pallas_call(
        functools.partial(grad_kernel, group, scale, inner, slots),
        out_shape=[jax.ShapeDtypeStruct(shape, BF16) for shape in outs],
        in_specs=[SMEM] + [VMEM] * (4 * slots + 1),
        out_specs=[VMEM] * len(outs),
        scratch_shapes=[
            pltpu.VMEM((blocks, width, rows), BF16),
            pltpu.VMEM((group, width, rows), F32),
            pltpu.VMEM((blocks, rows, width), F32),
            pltpu.VMEM((blocks, rows, width), F32),
        ],
        cost_estimate=pl.CostEstimate(flops=flops, bytes_accessed=q[0].size * 12, transcendentals=0),
        name="grads",
    )(table, *q, *do, *lse, *delta, kv)


def exchange(x, axes):
    return lax.all_to_all(x, axes, split_axis=0, concat_axis=0, tiled=True)


def partner(index, step, count):
    if count & (count - 1) == 0:
        return index ^ step
    return (step - index) % count


def trade(x, axis, step):
    count = lax.axis_size(axis)
    return lax.ppermute(x, axis, [(d, partner(d, step, count)) for d in range(count)])


def natural(pieces, index):
    count = len(pieces)

    def pick(place):
        kept = pieces[0]
        for step in range(1, count):
            kept = jnp.where(partner(index, step, count) == place, pieces[step], kept)
        return kept

    return [pick(place) for place in range(count)]


def body(query, keys, values, forward_output, d_out, span_order):
    rows, heads, width = query.shape
    kv_count = keys.shape[1]
    scale = width ** (-0.5)
    cores, inner, zs = lax.axis_size("outer"), lax.axis_size("inner"), lax.axis_size("head")
    core, place, z_in = (lax.axis_index(axis) for axis in ("outer", "inner", "head"))
    blocks = cores * inner
    own_heads = heads // cores
    shared = kv_count % cores != 0
    own_kv = 1 if shared else kv_count // cores
    group_heads = own_heads // own_kv
    slice_rows = rows // zs
    group = min(8, group_heads)

    kv = jnp.stack([jnp.moveaxis(keys, 1, 0), jnp.moveaxis(values, 1, 0)], axis=1)
    kv = jnp.broadcast_to(kv, (cores,) + kv.shape) if shared else kv.reshape((cores, own_kv) + kv.shape[1:])
    kv = jnp.broadcast_to(kv[:, None], (cores, inner) + kv.shape[1:])
    kv = exchange(kv.reshape((blocks,) + kv.shape[2:]), ("outer", "inner"))

    def share(x):
        x = jnp.moveaxis(x, 1, 0)
        x = x.reshape((cores, own_heads) + x.shape[1:])
        got = [lax.dynamic_index_in_dim(x, core, 0, keepdims=False)]
        for step in range(1, cores):
            out = lax.dynamic_index_in_dim(x, (core + step) % cores, 0, keepdims=False)
            got.append(lax.ppermute(out, "outer", [(d, (d + step) % cores) for d in range(cores)]))
        return [got[0]] + got[:0:-1]

    delta = jnp.sum(d_out.astype(F32) * forward_output.astype(F32), axis=-1)
    q_all, do_all, delta_all = share(query), share(d_out), share(delta)

    order = span_order[0]
    ids = jnp.arange(blocks, dtype=jnp.int32)
    by_place = jnp.sum(jnp.where(order[None, :] == ids[:, None], ids[None, :], 0), axis=1)
    own_blocks = (core + jnp.arange(cores, dtype=jnp.int32)) % cores * inner + place
    places = jnp.sum(jnp.where(own_blocks[:, None] == ids[None, :], order[None, :], 0), axis=1)
    table = jnp.concatenate([by_place, places, jnp.stack([core, place, z_in]).astype(jnp.int32)])

    dq, sums = [], []
    for g in range(own_kv):
        q, do, delta_g = (
            [part[g * group_heads : (g + 1) * group_heads] for part in x]
            for x in (q_all, do_all, delta_all)
        )
        lse = lse_call(table, q, kv[:, g], group, scale)
        dq_g, own, *others = grad_call(table, q, do, lse, delta_g, kv[:, g], group, scale, inner, zs)
        dq.append(dq_g)
        total = own.astype(F32)
        for step, part in enumerate(others, 1):
            part = trade(part, "inner", step)
            total = total + part.astype(F32)
        sums.append(total.astype(BF16))

    dq = exchange(jnp.concatenate(dq, axis=1), ("outer", "head"))
    dq = dq.reshape(cores, zs, own_heads, slice_rows, width)
    dq = jnp.transpose(dq, (3, 1, 0, 2, 4)).reshape(1, slice_rows, zs * heads, width)
    sums = jnp.stack(sums, axis=1)
    pieces = [[None] * cores for _ in range(zs)]
    for z in range(zs):
        for c in range(cores):
            pieces[z][c] = sums[c * zs + z]
            if z or c:
                pairs = []
                for d in range(zs * cores):
                    target = partner(d // cores, z, zs) * cores + partner(d % cores, c, cores)
                    pairs.append((d, target))
                pieces[z][c] = lax.ppermute(pieces[z][c], ("head", "outer"), pairs)
    pieces = natural([jnp.stack(natural(row, core)) for row in pieces], z_in)
    sums = jnp.stack(pieces, axis=1)
    if shared:
        sums = jnp.sum(sums.astype(F32), axis=0, keepdims=True).astype(BF16)
    sums = jnp.transpose(sums, (3, 4, 1, 0, 2, 5)).reshape(2, 1, slice_rows, zs * kv_count, width)
    return dq, sums[0], sums[1]


def solution(mesh):
    rows_spec = P(("outer", "inner"), "head", None)
    out_spec = P(("outer", "inner"), "head", None, None)
    return jax.shard_map(
        body,
        mesh=mesh,
        in_specs=(rows_spec,) * 5 + (P(),),
        out_specs=(out_spec,) * 3,
        check_vma=False,
    )
```

```python
import functools
import math

import jax
import jax.numpy as jnp
from jax import lax
from jax.experimental import pallas as pl
from jax.experimental.pallas import tpu as pltpu
from jax.sharding import PartitionSpec as P


F32 = jnp.float32
BF16 = jnp.bfloat16
NT = (((1,), (1,)), ((), ()))
NN = (((1,), (0,)), ((), ()))
MASKED = -1e30
VMEM = pl.BlockSpec(memory_space=pltpu.VMEM)
SMEM = pl.BlockSpec(memory_space=pltpu.SMEM)


def dot(a, b, dims):
    return lax.dot_general(a, b, dims, preferred_element_type=F32)


def causal_tile(rows):
    shape = (rows, rows)
    return lax.broadcasted_iota(jnp.int32, shape, 0) <= lax.broadcasted_iota(jnp.int32, shape, 1)


def over_visible(place, tile):
    tile(place, True)

    def turn(k, _):
        tile(k, False)
        return 0

    lax.fori_loop(0, place, turn, 0)


def grad_kernel(group, chunk, scale, slots, inner, table, *refs):
    q_refs, do_refs, delta_refs = (refs[k * slots : (k + 1) * slots] for k in range(3))
    kv_ref, dq_ref = refs[3 * slots], refs[3 * slots + 1]
    out_refs = refs[3 * slots + 2 : -9]
    kt_ref, x_ref, m_ref, l_ref, dqt_ref, dka_ref, dva_ref, p_ref, ds_ref = refs[-9:]
    heads, rows, width = q_refs[0].shape
    blocks = kv_ref.shape[0]
    slice_rows = dq_ref.shape[2]
    zs = rows // slice_rows
    scale2 = scale * math.log2(math.e)
    causal = causal_tile(rows)
    core, place_in, z_in = (table[blocks + slots + k] for k in range(3))
    dka_ref[...] = jnp.zeros_like(dka_ref)
    dva_ref[...] = jnp.zeros_like(dva_ref)
    for b in range(blocks):
        kt_ref[b] = kv_ref[b, 0].T
    for s in range(slots):
        q_ref, do_ref, delta_ref = q_refs[s], do_refs[s], delta_refs[s]
        place = table[blocks + s]
        for g in range(0, heads, group):

            def totals(k, diag):
                keys = kv_ref[table[k], 0]
                for j in range(group):
                    x = dot(keys, q_ref[g + j], NT) * scale2
                    if diag:
                        x = jnp.where(causal, x, MASKED)
                    x_ref[k, j] = x
                    x = x.reshape(rows // 8, 8, rows)
                    m_new = jnp.max(x, axis=0)
                    if not diag:
                        m_old = m_ref[j]
                        m_new = jnp.maximum(m_old, m_new)
                    total = jnp.sum(jnp.exp2(x - m_new[None]), axis=0)
                    if not diag:
                        total = total + l_ref[j] * jnp.exp2(m_old - m_new)
                    m_ref[j] = m_new
                    l_ref[j] = total

            over_visible(place, totals)
            for j in range(group):
                m = m_ref[j]
                high = jnp.max(m, axis=0, keepdims=True)
                total = jnp.sum(l_ref[j] * jnp.exp2(m - high), axis=0, keepdims=True)
                m_ref[j] = jnp.broadcast_to(high + jnp.log2(total), (8, rows))

            def tile(k, diag):
                block = table[k]
                for j in range(group):
                    lse_row, delta_row = m_ref[j, 0:1], delta_ref[g + j : g + j + 1, :]
                    head = slice(j * rows, (j + 1) * rows)
                    for c in range(0, rows, chunk):
                        cut = slice(c, c + chunk)
                        dp = dot(kv_ref[block, 1, cut], do_ref[g + j], NT)
                        p = jnp.exp2(x_ref[k, j, cut] - lse_row)
                        p_ref[cut, head] = p.astype(BF16)
                        ds_ref[cut, head] = (p * (dp - delta_row)).astype(BF16)
                keys_t = kt_ref[block]
                for j in range(group):
                    part = dot(keys_t, ds_ref[:, j * rows : (j + 1) * rows], NN)
                    if diag:
                        dqt_ref[j] = part
                    else:
                        dqt_ref[j] += part
                wide = slice(g, g + group)
                dva_ref[block] += dot(p_ref[...], do_ref[wide].reshape(group * rows, width), NN)
                dka_ref[block] += dot(ds_ref[...], q_ref[wide].reshape(group * rows, width), NN)

            over_visible(place, tile)
            to_core = lax.rem(core + s, slots)
            for j in range(group):
                dq = (dqt_ref[j] * scale).T.astype(BF16)
                for z in range(zs):
                    dq_ref[to_core * zs + z, g + j] = dq[z * slice_rows : (z + 1) * slice_rows]
    for step, out_ref in enumerate(out_refs):
        block = partner(core, step // inner, slots) * inner + partner(place_in, step % inner, inner)
        for z in range(zs):
            start = pl.multiple_of(partner(z_in, z, zs) * slice_rows, slice_rows)
            cut = pl.ds(start, slice_rows)
            out_ref[z, 0] = (dka_ref[block, cut] * scale).astype(BF16)
            out_ref[z, 1] = dva_ref[block, cut].astype(BF16)


def grad_call(table, q, do, delta, kv, group, scale, inner, zs):
    heads, rows, width = q[0].shape
    slots, blocks = len(q), kv.shape[0]
    slice_rows = rows // zs
    chunk = rows // 2
    flops = 5 * slots * heads * rows * rows * blocks * width
    outs = [(slots * zs, heads, slice_rows, width)] + [(zs, 2, slice_rows, width)] * blocks
    return pl.pallas_call(
        functools.partial(grad_kernel, group, chunk, scale, slots, inner),
        out_shape=[jax.ShapeDtypeStruct(shape, BF16) for shape in outs],
        in_specs=[SMEM] + [VMEM] * (3 * slots + 1),
        out_specs=[VMEM] * len(outs),
        scratch_shapes=[
            pltpu.VMEM((blocks, width, rows), BF16),
            pltpu.VMEM((blocks, group, rows, rows), F32),
            pltpu.VMEM((group, 8, rows), F32),
            pltpu.VMEM((group, 8, rows), F32),
            pltpu.VMEM((group, width, rows), F32),
            pltpu.VMEM((blocks, rows, width), F32),
            pltpu.VMEM((blocks, rows, width), F32),
            pltpu.VMEM((rows, group * rows), BF16),
            pltpu.VMEM((rows, group * rows), BF16),
        ],
        cost_estimate=pl.CostEstimate(flops=flops, bytes_accessed=q[0].size * 12, transcendentals=0),
        name="grads",
    )(table, *q, *do, *delta, kv)


def exchange(x, axes):
    return lax.all_to_all(x, axes, split_axis=0, concat_axis=0, tiled=True)


def partner(index, step, count):
    if count & (count - 1) == 0:
        return index ^ step
    return (step - index) % count


def trade(x, axes, steps):
    counts = [lax.axis_size(axis) for axis in axes]
    pairs = []
    for device in range(math.prod(counts)):
        target, rest = 0, device
        places = []
        for count in reversed(counts):
            places.insert(0, rest % count)
            rest //= count
        for spot, step, count in zip(places, steps, counts):
            target = target * count + partner(spot, step, count)
        pairs.append((device, target))
    return lax.ppermute(x, axes, pairs)


def natural(pieces, index):
    count = len(pieces)

    def pick(place):
        kept = pieces[0]
        for step in range(1, count):
            kept = jnp.where(partner(index, step, count) == place, pieces[step], kept)
        return kept

    return [pick(place) for place in range(count)]


def body(query, keys, values, forward_output, d_out, span_order):
    rows, heads, width = query.shape
    kv_count = keys.shape[1]
    scale = width ** (-0.5)
    cores, inner, zs = lax.axis_size("outer"), lax.axis_size("inner"), lax.axis_size("head")
    core, place, z_in = (lax.axis_index(axis) for axis in ("outer", "inner", "head"))
    blocks = cores * inner
    own_heads = heads // cores
    shared = kv_count % cores != 0
    own_kv = 1 if shared else kv_count // cores
    group_heads = own_heads // own_kv
    slice_rows = rows // zs
    group = max(1, min(8, group_heads, 64 // blocks))

    kv = jnp.stack([jnp.moveaxis(keys, 1, 0), jnp.moveaxis(values, 1, 0)], axis=1)
    kv = jnp.broadcast_to(kv, (cores,) + kv.shape) if shared else kv.reshape((cores, own_kv) + kv.shape[1:])
    kv = jnp.broadcast_to(kv[:, None], (cores, inner) + kv.shape[1:])
    kv = exchange(kv.reshape((blocks,) + kv.shape[2:]), ("outer", "inner"))

    def share(x):
        x = jnp.moveaxis(x, 1, 0)
        x = x.reshape((cores, own_heads) + x.shape[1:])
        got = [lax.dynamic_index_in_dim(x, core, 0, keepdims=False)]
        for step in range(1, cores):
            out = lax.dynamic_index_in_dim(x, (core + step) % cores, 0, keepdims=False)
            got.append(lax.ppermute(out, "outer", [(d, (d + step) % cores) for d in range(cores)]))
        return [got[0]] + got[:0:-1]

    delta = jnp.sum(d_out.astype(F32) * forward_output.astype(F32), axis=-1)
    q_all, do_all, delta_all = share(query), share(d_out), share(delta)

    order = span_order[0]
    ids = jnp.arange(blocks, dtype=jnp.int32)
    by_place = jnp.sum(jnp.where(order[None, :] == ids[:, None], ids[None, :], 0), axis=1)
    own_blocks = (core + jnp.arange(cores, dtype=jnp.int32)) % cores * inner + place
    places = jnp.sum(jnp.where(own_blocks[:, None] == ids[None, :], order[None, :], 0), axis=1)
    table = jnp.concatenate([by_place, places, jnp.stack([core, place, z_in]).astype(jnp.int32)])

    dq, pieces = [], []
    for g in range(own_kv):
        mine = slice(g * group_heads, (g + 1) * group_heads)
        q, do, delta_g = ([part[mine] for part in x] for x in (q_all, do_all, delta_all))
        dq_g, *pieces_g = grad_call(table, q, do, delta_g, kv[:, g], group, scale, inner, zs)
        dq.append(dq_g)
        pieces.append(pieces_g)
    pieces = [jnp.stack(part, axis=1) for part in zip(*pieces)]

    sums = [None] * cores
    for step, part in enumerate(pieces):
        c, i = divmod(step, inner)
        if step:
            part = trade(part, ("outer", "inner"), (c, i))
        part = part.astype(F32)
        sums[c] = part if sums[c] is None else sums[c] + part
    if shared:
        sums = [sum(sums)]
    else:
        sums = natural(sums, core)
    sums = jnp.concatenate(sums, axis=1).astype(BF16)

    dq = exchange(jnp.concatenate(dq, axis=1), ("outer", "head"))
    dq = dq.reshape(cores, zs, own_heads, slice_rows, width)
    dq = jnp.transpose(dq, (3, 1, 0, 2, 4)).reshape(1, slice_rows, zs * heads, width)
    got = [sums[0]]
    for z in range(1, zs):
        got.append(trade(sums[z], ("head",), (z,)))
    sums = jnp.stack(natural(got, z_in))
    sums = jnp.transpose(sums, (2, 3, 0, 1, 4)).reshape(2, 1, slice_rows, zs * kv_count, width)
    return dq, sums[0], sums[1]


def solution(mesh):
    rows_spec = P(("outer", "inner"), "head", None)
    out_spec = P(("outer", "inner"), "head", None, None)
    return jax.shard_map(
        body,
        mesh=mesh,
        in_specs=(rows_spec,) * 5 + (P(),),
        out_specs=(out_spec,) * 3,
        check_vma=False,
    )
```

```python
import functools
import math

import jax
import jax.numpy as jnp
from jax import lax
from jax.experimental import pallas as pl
from jax.experimental.pallas import tpu as pltpu
from jax.sharding import PartitionSpec as P


F32 = jnp.float32
BF16 = jnp.bfloat16
NT = (((1,), (1,)), ((), ()))
NN = (((1,), (0,)), ((), ()))
MASKED = -1e30
VMEM = pl.BlockSpec(memory_space=pltpu.VMEM)
SMEM = pl.BlockSpec(memory_space=pltpu.SMEM)


def dot(a, b, dims):
    return lax.dot_general(a, b, dims, preferred_element_type=F32)


def causal_tile(rows):
    shape = (rows, rows)
    return lax.broadcasted_iota(jnp.int32, shape, 0) <= lax.broadcasted_iota(jnp.int32, shape, 1)


def over_visible(place, tile):
    tile(place, True)

    def turn(k, _):
        tile(k, False)
        return 0

    lax.fori_loop(0, place, turn, 0)


def grad_kernel(group, chunk, scale, slot, slots, inner, zs, table, *refs):
    q_ref, do_ref, delta_ref, kv_ref = refs[:4]
    first, last = slot == 0, slot == slots - 1
    start_refs, refs = ((), refs[4:]) if first else (refs[4:6], refs[6:])
    dq_refs, out_refs = refs[:zs], refs[zs:-10]
    kt_ref, x_ref, m_ref, l_ref, dqt_ref, dka_ref, dva_ref, p_ref, ds_ref, turned_ref = refs[-10:]
    heads, rows, width = q_ref.shape
    blocks = kv_ref.shape[0]
    slice_rows = rows // zs
    scale2 = scale * math.log2(math.e)
    causal = causal_tile(rows)
    core, place_in, z_in = (table[blocks + slots + index] for index in range(3))
    for acc_ref, index in ((dka_ref, 0), (dva_ref, 1)):
        acc_ref[...] = jnp.zeros_like(acc_ref) if first else start_refs[index][...]
    for b in range(blocks):
        kt_ref[b] = kv_ref[b, 0].T
    place = table[blocks + slot]
    for g in range(0, heads, group):

        def totals(k, diag):
            keys = kv_ref[table[k], 0]
            for j in range(group):
                x = dot(keys, q_ref[g + j], NT) * scale2
                if diag:
                    x = jnp.where(causal, x, MASKED)
                x_ref[k, j] = x
                x = x.reshape(rows // 8, 8, rows)
                m_new = jnp.max(x, axis=0)
                if not diag:
                    m_old = m_ref[j]
                    m_new = jnp.maximum(m_old, m_new)
                total = jnp.sum(jnp.exp2(x - m_new[None]), axis=0)
                if not diag:
                    total = total + l_ref[j] * jnp.exp2(m_old - m_new)
                m_ref[j] = m_new
                l_ref[j] = total

        over_visible(place, totals)
        for j in range(group):
            m = m_ref[j]
            high = jnp.max(m, axis=0, keepdims=True)
            total = jnp.sum(l_ref[j] * jnp.exp2(m - high), axis=0, keepdims=True)
            m_ref[j] = jnp.broadcast_to(high + jnp.log2(total), (8, rows))

        def tile(k, diag):
            block = table[k]
            for j in range(group):
                lse_row, delta_row = m_ref[j, 0:1], delta_ref[g + j : g + j + 1, :]
                head = slice(j * rows, (j + 1) * rows)
                for c in range(0, rows, chunk):
                    cut = slice(c, c + chunk)
                    dp = dot(kv_ref[block, 1, cut], do_ref[g + j], NT)
                    p = jnp.exp2(x_ref[k, j, cut] - lse_row)
                    p_ref[cut, head] = p.astype(BF16)
                    ds_ref[cut, head] = (p * (dp - delta_row)).astype(BF16)
            keys_t = kt_ref[block]
            for j in range(group):
                part = dot(keys_t, ds_ref[:, j * rows : (j + 1) * rows], NN)
                if diag:
                    dqt_ref[j] = part
                else:
                    dqt_ref[j] += part
            wide = slice(g, g + group)
            dva_ref[block] += dot(p_ref[...], do_ref[wide].reshape(group * rows, width), NN)
            dka_ref[block] += dot(ds_ref[...], q_ref[wide].reshape(group * rows, width), NN)

        over_visible(place, tile)
        for j in range(group):
            turned_ref[...] = (dqt_ref[j] * scale).T
            for z in range(zs):
                start = pl.multiple_of(partner(z_in, z, zs) * slice_rows, slice_rows)
                dq_refs[z][g + j] = turned_ref[pl.ds(start, slice_rows)].astype(BF16)
    if not last:
        out_refs[0][...] = dka_ref[...]
        out_refs[1][...] = dva_ref[...]
        return
    for step, out_ref in enumerate(out_refs):
        block = partner(core, step // inner, slots) * inner + partner(place_in, step % inner, inner)
        for z in range(zs):
            start = pl.multiple_of(partner(z_in, z, zs) * slice_rows, slice_rows)
            cut = pl.ds(start, slice_rows)
            out_ref[z, 0] = (dka_ref[block, cut] * scale).astype(BF16)
            out_ref[z, 1] = dva_ref[block, cut].astype(BF16)


def grad_call(table, q, do, delta, kv, sums, group, scale, slot, slots, inner, zs):
    heads, rows, width = q.shape
    blocks = kv.shape[0]
    slice_rows = rows // zs
    flops = 5 * heads * rows * rows * blocks * width
    total = (blocks, rows, width)
    outs = [jax.ShapeDtypeStruct((heads, slice_rows, width), BF16)] * zs
    if slot < slots - 1:
        outs += [jax.ShapeDtypeStruct(total, F32)] * 2
    else:
        outs += [jax.ShapeDtypeStruct((zs, 2, slice_rows, width), BF16)] * blocks
    out = pl.pallas_call(
        functools.partial(grad_kernel, group, rows // 2, scale, slot, slots, inner, zs),
        out_shape=outs,
        in_specs=[SMEM] + [VMEM] * (4 + len(sums)),
        out_specs=[VMEM] * len(outs),
        scratch_shapes=[
            pltpu.VMEM((blocks, width, rows), BF16),
            pltpu.VMEM((blocks, group, rows, rows), F32),
            pltpu.VMEM((group, 8, rows), F32),
            pltpu.VMEM((group, 8, rows), F32),
            pltpu.VMEM((group, width, rows), F32),
            pltpu.VMEM(total, F32),
            pltpu.VMEM(total, F32),
            pltpu.VMEM((rows, group * rows), BF16),
            pltpu.VMEM((rows, group * rows), BF16),
            pltpu.VMEM((rows, width), F32),
        ],
        cost_estimate=pl.CostEstimate(flops=flops, bytes_accessed=q.size * 12, transcendentals=0),
    )(table, q, do, delta, kv, *sums)
    return out[:zs], out[zs:]


def exchange(x, axes):
    return lax.all_to_all(x, axes, split_axis=0, concat_axis=0, tiled=True)


def partner(index, step, count):
    if count & (count - 1) == 0:
        return index ^ step
    return (step - index) % count


def trade(x, axes, steps):
    counts = [lax.axis_size(axis) for axis in axes]
    pairs = []
    for device in range(math.prod(counts)):
        target, rest = 0, device
        places = []
        for count in reversed(counts):
            places.insert(0, rest % count)
            rest //= count
        for spot, step, count in zip(places, steps, counts):
            target = target * count + partner(spot, step, count)
        pairs.append((device, target))
    return lax.ppermute(x, axes, pairs)


def natural(pieces, index):
    count = len(pieces)

    def pick(place):
        kept = pieces[0]
        for step in range(1, count):
            kept = jnp.where(partner(index, step, count) == place, pieces[step], kept)
        return kept

    return [pick(place) for place in range(count)]


def body(query, keys, values, forward_output, d_out, span_order):
    rows, heads, width = query.shape
    kv_count = keys.shape[1]
    scale = width ** (-0.5)
    cores, inner, zs = lax.axis_size("outer"), lax.axis_size("inner"), lax.axis_size("head")
    core, place, z_in = (lax.axis_index(axis) for axis in ("outer", "inner", "head"))
    blocks = cores * inner
    own_heads = heads // cores
    shared = kv_count % cores != 0
    own_kv = 1 if shared else kv_count // cores
    group_heads = own_heads // own_kv
    slice_rows = rows // zs
    group = max(1, min(8, group_heads, 64 // blocks))

    kv = jnp.stack([jnp.moveaxis(keys, 1, 0), jnp.moveaxis(values, 1, 0)], axis=1)
    kv = jnp.broadcast_to(kv, (cores,) + kv.shape) if shared else kv.reshape((cores, own_kv) + kv.shape[1:])
    kv = jnp.broadcast_to(kv[:, None], (cores, inner) + kv.shape[1:])
    kv = exchange(kv.reshape((blocks,) + kv.shape[2:]), ("outer", "inner"))

    def share(x):
        x = jnp.moveaxis(x, 1, 0)
        x = x.reshape((cores, own_heads) + x.shape[1:])
        got = [lax.dynamic_index_in_dim(x, core, 0, keepdims=False)]
        for step in range(1, cores):
            away = lax.dynamic_index_in_dim(x, partner(core, step, cores), 0, keepdims=False)
            got.append(trade(away, ("outer",), (step,)))
        return got

    delta = jnp.sum(d_out.astype(F32) * forward_output.astype(F32), axis=-1)
    q_all, do_all, delta_all = share(query), share(d_out), share(delta)

    order = span_order[0]
    ids = jnp.arange(blocks, dtype=jnp.int32)
    by_place = jnp.sum(jnp.where(order[None, :] == ids[:, None], ids[None, :], 0), axis=1)
    own_blocks = jnp.stack([partner(core, step, cores) for step in range(cores)]) * inner + place
    places = jnp.sum(jnp.where(own_blocks[:, None] == ids[None, :], order[None, :], 0), axis=1)
    table = jnp.concatenate([by_place, places, jnp.stack([core, place, z_in]).astype(jnp.int32)])

    sums = [()] * own_kv
    dq = []
    for slot in range(cores):
        parts = []
        for g in range(own_kv):
            mine = slice(g * group_heads, (g + 1) * group_heads)
            operands = (x[slot][mine] for x in (q_all, do_all, delta_all))
            part, sums[g] = grad_call(
                table, *operands, kv[:, g], sums[g], group, scale, slot, cores, inner, zs
            )
            parts.append(part)
        parts = [jnp.concatenate(part, axis=0) for part in zip(*parts)]
        got = []
        for z in range(zs):
            got.append(trade(parts[z], ("head", "outer"), (z, slot)) if z or slot else parts[z])
        dq.append(jnp.stack(natural(got, z_in)))
    dq = jnp.stack(natural(dq, core), axis=1)
    dq = jnp.transpose(dq, (3, 0, 1, 2, 4)).reshape(1, slice_rows, zs * heads, width)
    pieces = [jnp.stack(part, axis=1) for part in zip(*sums)]

    sums = [None] * cores
    for step, part in enumerate(pieces):
        c, i = divmod(step, inner)
        if step:
            part = trade(part, ("outer", "inner"), (c, i))
        part = part.astype(F32)
        sums[c] = part if sums[c] is None else sums[c] + part
    if shared:
        sums = [sum(sums)]
    else:
        sums = natural(sums, core)
    sums = jnp.concatenate(sums, axis=1).astype(BF16)

    got = [sums[0]]
    for z in range(1, zs):
        got.append(trade(sums[z], ("head",), (z,)))
    sums = jnp.stack(natural(got, z_in))
    sums = jnp.transpose(sums, (2, 3, 0, 1, 4)).reshape(2, 1, slice_rows, zs * kv_count, width)
    return dq, sums[0], sums[1]


def solution(mesh):
    rows_spec = P(("outer", "inner"), "head", None)
    out_spec = P(("outer", "inner"), "head", None, None)
    return jax.shard_map(
        body,
        mesh=mesh,
        in_specs=(rows_spec,) * 5 + (P(),),
        out_specs=(out_spec,) * 3,
        check_vma=False,
    )
```
